32 devices in a mesh: group: 2 (over x), expert: 16 (over z, y, core).
Axes of the slice: x: 2, y: 2, z: 4, core: 2. Of those that a mesh axis runs over, the one named last changes fastest.
Arguments:
- rows: bfloat16 [4096, 1024], P(('group', 'expert')), parts along dimension 0, may hold values from -6 to 6
- cotangent: bfloat16 [4096, 1024], P(('group', 'expert')), parts along dimension 0, may hold values from -1.5 to 1.5
- up_proj: bfloat16 [1024, 65536], P(None, 'expert'), may hold values from -0.1875 to 0.1875
- down_proj: bfloat16 [65536, 1024], P('expert'), may hold values from -0.125 to 0.125
- mix_weight: float32 [8, 4], replicated, may hold values from 0.25 to 1
- task_counts: int32 [32, 8], P(('group', 'expert')), parts along dimension 0, may hold values from 1 to 18, 128 in all within a row
- expert_order: int32 [32, 32], P(('group', 'expert')), parts along dimension 0, may hold values from 0 to 31, each once within a row
Outputs:
- mixed: bfloat16 [4096, 1024], P(('group', 'expert')), parts along dimension 0
- row_gradient: bfloat16 [4096, 1024], P(('group', 'expert')), parts along dimension 0
- up_grad: bfloat16 [2048, 65536], P('group', 'expert'), parts along dimension 0
- down_grad: bfloat16 [65536, 2048], P('expert', 'group'), parts along dimension 1
The draws below stay inside these ranges and needn't reach their ends.
There are 2 independent parts, one for each index of `group`. The reference program is written for one: setup_inputs(seed, part) draws one part's arguments, and reference() takes and returns one part's arrays. A program takes and returns all parts, laid end to end along the dimension named above; an argument that names none is the same for every part. Nothing has to cross between parts.
Inputs may be any that keep to these rules, and one draw needn't show every extreme that they name: `task_counts`: in each block the 8 counts sum to 128, and one of them is exactly 18. Each row of expert_order names every expert once.
All inputs are finite; a program needn't handle non-finite values.
Results may differ from the reference program's by a relative error of at most 0.0085.
Values may be sent and summed in bfloat16 or wider, within the bound.
No kernel may reach another device: no remote copies, remote signals or barrier semaphores. Data moves between devices by JAX's collectives and lax.ppermute only.
A program may use at most 128 MiB of HBM per device.

```python
import math
from functools import partial
import jax
import jax.numpy as jnp
import numpy as np
from jax import lax

D = 1024
FF = 2048
EXPERTS = 32
TASKS = 8
K = 4
TOKEN_BLOCK_ROWS = 128
CAP = 18
ROWS = 2048
N_EXPERT = 16


def steps_of(own_key, dims, cuts, smallest, top_value):
    level, own = 1.0, jax.random.fold_in(own_key, 6)
    for dim, blocks in cuts:
        draws = jnp.exp(jax.random.uniform(jax.random.fold_in(own, dim), (blocks,), jnp.float32, smallest / len(cuts), top_value / len(cuts)))
        level = level * jnp.repeat(draws, dims[dim] // blocks).reshape([-1 if axis == dim else 1 for axis in range(len(dims))])
    return level


def length_profile(amount, total, reach, skew):
    loads = [(1 << 20) // math.isqrt(rank ** skew) + 1 for rank in range(2, amount + 1)]
    spare, given = total - reach - (amount - 1), [1] * (amount - 1)
    while spare > 0:
        movable = [i for i in range(amount - 1) if given[i] < reach]
        whole, remaining = sum([loads[i] for i in movable]), spare
        for i in movable:
            more = min(reach - given[i], max(1, remaining * loads[i] // whole), spare)
            given[i] = given[i] + more
            spare = spare - more
    return np.array([reach] + given)


def uneven_parts(rng, amount, total, limit, slope):
    if amount == 2:
        one = jax.random.randint(rng, (), max(1, total - limit), min(limit, total - 1) + 1)
        return jnp.stack([one, total - one])
    sizes = jnp.asarray(length_profile(amount, total, limit, slope), jnp.int32)
    couples = (amount - 1) // 2
    source_of, receiver = sizes[1:1 + 2 * couples:2], sizes[2:2 + 2 * couples:2]
    room = jnp.minimum(source_of - 1, limit - receiver)
    shifted = jax.random.randint(jax.random.fold_in(rng, 1), (couples,), 0, 1 << 20) % (room + 1)
    sizes = sizes.at[1:1 + 2 * couples:2].set(source_of - shifted).at[2:2 + 2 * couples:2].set(receiver + shifted)
    return sizes[jax.random.permutation(jax.random.fold_in(rng, 2), amount)]


def gaussian(key, shape, width, most, split=(), kind=jnp.bfloat16):
    result = jax.random.normal(key, shape, jnp.float32) * width
    if len(split) > 0:
        result = steps_of(key, shape, split, -0.22, 0.18) * result
    return jnp.clip(result, min=-most, max=most).astype(kind)


def setup_inputs(seed: int = 0, part: int = 0) -> dict:
    streams_of = jax.random.split(jax.random.key(seed), 8)
    part_splits = jax.random.split(jax.random.fold_in(streams_of[7], part), 8)
    rows = gaussian(part_splits[0], (ROWS, D), 1.0, 6.0, ((0, 16),))
    cotangent = gaussian(part_splits[1], (ROWS, D), 0.25, 1.5, ((0, 16),))
    up_proj = gaussian(streams_of[2], (D, EXPERTS * FF), D ** -0.5, 0.1875, ((1, 16),))
    down_proj = gaussian(streams_of[3], (EXPERTS * FF, D), FF ** -0.5, 0.125, ((0, 16),))
    mix_weight = jnp.clip(jnp.exp(jax.random.uniform(streams_of[4], (TASKS, K), jnp.float32, math.log(0.25), math.log(1.0))), 0.25, 1.0)
    task_counts = jax.vmap(lambda own: uneven_parts(own, TASKS, TOKEN_BLOCK_ROWS, CAP, 2))(jax.random.split(part_splits[5], N_EXPERT)).reshape((N_EXPERT, TASKS)).astype(jnp.int32)
    expert_order = jax.vmap(lambda own: jax.random.permutation(own, EXPERTS))(jax.random.split(part_splits[6], N_EXPERT)).reshape((N_EXPERT, EXPERTS)).astype(jnp.int32)
    return {"rows": rows, "cotangent": cotangent, "up_proj": up_proj, "down_proj": down_proj, "mix_weight": mix_weight, "task_counts": task_counts, "expert_order": expert_order}


def block_route(counts, expert_list, mix_flat, row_total):
    counts = counts.astype(jnp.int32)
    firsts = (jnp.cumsum(counts) - counts).astype(jnp.int32)
    labels = jnp.arange(EXPERTS, dtype=jnp.int32)
    matches = expert_list[None, :].astype(jnp.int32) == labels[:, None]
    position = jnp.sum(jnp.where(matches, labels[None, :], 0), axis=1).astype(jnp.int32)
    task_of = position // K
    task_match = task_of[:, None] == jnp.arange(TASKS, dtype=jnp.int32)[None, :]
    count_of = jnp.sum(jnp.where(task_match, counts[None, :], 0), axis=1).astype(jnp.int32)
    first_of = jnp.sum(jnp.where(task_match, firsts[None, :], 0), axis=1).astype(jnp.int32)
    weight_of = jnp.sum(jnp.where(matches, mix_flat[None, :], jnp.zeros_like(mix_flat)[None, :]), axis=1)
    slot_index = jnp.arange(CAP, dtype=jnp.int32)
    filled = slot_index[None, :] < count_of[:, None]
    targets = first_of[:, None] + slot_index[None, :]
    row_index = jnp.arange(row_total, dtype=jnp.int32)
    selection_index = (targets[:, :, None] == row_index[None, None, :]) & filled[:, :, None]
    selection_index = selection_index.reshape(EXPERTS * CAP, row_total).astype(jnp.float32)
    slot_weight = jnp.where(filled, weight_of[:, None], jnp.zeros_like(weight_of)[:, None]).reshape(-1)
    return selection_index, slot_weight


def expert_step(operands):
    inputs, scaled, up_slice, down_slice = operands
    pre = jnp.dot(inputs, up_slice, preferred_element_type=jnp.float32)
    act = jax.nn.silu(pre).astype(jnp.bfloat16)
    outputs = jnp.dot(act, down_slice, preferred_element_type=jnp.float32)
    act_grad = jnp.dot(scaled, down_slice.T, preferred_element_type=jnp.float32)
    sigmoid = jax.nn.sigmoid(pre)
    pre_grad = (act_grad * sigmoid * (1.0 + pre * (1.0 - sigmoid))).astype(jnp.bfloat16)
    down_part = jnp.dot(act.T, scaled, preferred_element_type=jnp.float32).astype(jnp.bfloat16)
    up_part = jnp.dot(inputs.T, pre_grad, preferred_element_type=jnp.float32).astype(jnp.bfloat16)
    input_grad = jnp.dot(pre_grad, up_slice.T, preferred_element_type=jnp.float32)
    return outputs, input_grad, up_part, down_part


def reference(rows, cotangent, up_proj, down_proj, mix_weight, task_counts, expert_order):
    block_list = N_EXPERT
    hidden_width = rows.shape[1]
    route = partial(block_route, row_total=TOKEN_BLOCK_ROWS)
    selection_index, slot_weight = jax.vmap(route, in_axes=(0, 0, None))(task_counts, expert_order, mix_weight.reshape(-1))
    row_block_list = rows.reshape(block_list, TOKEN_BLOCK_ROWS, hidden_width).astype(jnp.float32)
    gradient_block_list = cotangent.reshape(block_list, TOKEN_BLOCK_ROWS, hidden_width).astype(jnp.float32)
    upper_bound = lax.Precision.HIGHEST
    slot_row_values = jnp.einsum('slt,stn->sln', selection_index, row_block_list, precision=upper_bound).astype(jnp.bfloat16)
    slot_gradient_rows = jnp.einsum('slt,stn->sln', selection_index, gradient_block_list, precision=upper_bound)
    scaled = (slot_weight[:, :, None] * slot_gradient_rows).astype(jnp.bfloat16)

    def by_expert(values):
        return values.reshape(block_list, EXPERTS, CAP, hidden_width).transpose(1, 0, 2, 3).reshape(EXPERTS, block_list * CAP, hidden_width)

    def grouped_per_block(values):
        return values.reshape(EXPERTS, block_list, CAP, hidden_width).transpose(1, 0, 2, 3).reshape(block_list, EXPERTS * CAP, hidden_width)

    up_slices = up_proj.reshape(hidden_width, EXPERTS, FF).transpose(1, 0, 2)
    down_slices = down_proj.reshape(EXPERTS, FF, hidden_width)
    outputs, input_gradient_rows, up_parts, down_parts = lax.map(expert_step, (by_expert(slot_row_values), by_expert(scaled), up_slices, down_slices))
    weighted_rows = grouped_per_block(outputs) * slot_weight[:, :, None]
    mixed = jnp.einsum('fua,ful->fal', selection_index, weighted_rows, precision=upper_bound).reshape(block_list * TOKEN_BLOCK_ROWS, hidden_width)
    row_gradient = jnp.einsum('fua,ful->fal', selection_index, grouped_per_block(input_gradient_rows), precision=upper_bound).reshape(block_list * TOKEN_BLOCK_ROWS, hidden_width)
    up_grad = up_parts.transpose(1, 0, 2).reshape(hidden_width, EXPERTS * FF)
    down_grad = down_parts.reshape(EXPERTS * FF, hidden_width)
    return mixed.astype(jnp.bfloat16), row_gradient.astype(jnp.bfloat16), up_grad, down_grad
```

```python
import functools

import jax
import jax.numpy as jnp
from jax import lax
from jax.experimental import pallas as pl
from jax.experimental.pallas import tpu as pltpu
from jax.sharding import PartitionSpec as P

FF = 2048
EXPERTS = 32
TASKS = 8
K = 4
CAP = 18
AUX = 8
LANES = 128
BF = jnp.bfloat16
F32 = jnp.float32


def plane_of(owners):
    return 1 << ((owners.bit_length() - 1) // 2)


def hop(value, mask, owners):
    return lax.ppermute(value, "expert", [(i, i ^ mask) for i in range(owners)])


def params(limit_mib=40):
    return pltpu.CompilerParams(vmem_limit_bytes=limit_mib << 20)


def cost(flops, moved):
    return pl.CostEstimate(flops=int(flops), bytes_accessed=int(moved), transcendentals=0)


def prep_kernel(rows_ref, counts_ref, order_ref, out_ref):
    row_total = rows_ref.shape[0]
    out_ref[:row_total, :] = rows_ref[...]
    width = out_ref.shape[1]
    lane = lax.broadcasted_iota(jnp.int32, (1, width), 1)
    first_of = jnp.zeros((1, width), jnp.int32)
    count_of = jnp.zeros((1, width), jnp.int32)
    total = jnp.int32(0)
    for t in range(TASKS):
        here = (lane >= t * K) & (lane < (t + 1) * K)
        count = counts_ref[0, t]
        first_of = jnp.where(here, total, first_of)
        count_of = jnp.where(here, count, count_of)
        total = total + count
    order = jnp.concatenate(
        [order_ref[...], jnp.full((1, width - EXPERTS), -1, jnp.int32)], axis=1
    )
    sub = lax.broadcasted_iota(jnp.int32, (AUX, width), 0)
    aux = jnp.where(
        sub == 0, order, jnp.where(sub == 1, first_of, jnp.where(sub == 2, count_of, 0))
    )
    out_ref[row_total:, :] = aux.astype(F32).astype(BF)


def prep(rows, counts, order):
    row_total, width = rows.shape
    return pl.pallas_call(
        prep_kernel,
        out_shape=jax.ShapeDtypeStruct((row_total + AUX, width), BF),
        in_specs=[
            pl.BlockSpec(memory_space=pltpu.VMEM),
            pl.BlockSpec(memory_space=pltpu.SMEM),
            pl.BlockSpec(memory_space=pltpu.VMEM),
        ],
        out_specs=pl.BlockSpec(memory_space=pltpu.VMEM),
        compiler_params=params(),
        cost_estimate=cost(1e6, 4 * rows.size),
        name="prep",
    )(rows, counts, order)


def slot_map(aux_refs, weight_ref, first_expert, local_count, row_total):
    blocks = len(aux_refs)
    group = blocks * CAP
    slots = local_count * group
    q = lax.broadcasted_iota(jnp.int32, (slots, LANES), 0)
    expert = sum((q >= e * group).astype(jnp.int32) for e in range(1, local_count)) + jnp.zeros_like(q)
    rest = q - expert * group
    block = sum((rest >= b * CAP).astype(jnp.int32) for b in range(1, blocks)) + jnp.zeros_like(q)
    slot = rest - block * CAP
    order = first = count = jnp.zeros((slots, LANES), F32)
    for b in range(blocks):
        aux = aux_refs[b][...].astype(F32)
        order = jnp.where(block == b, aux[0:1, :LANES], order)
        first = jnp.where(block == b, aux[1:2, :LANES], first)
        count = jnp.where(block == b, aux[2:3, :LANES], count)
    match = order == (expert + first_expert).astype(F32)
    first = jnp.sum(jnp.where(match, first, 0.0), axis=1, keepdims=True)
    count = jnp.sum(jnp.where(match, count, 0.0), axis=1, keepdims=True)
    slot_of = slot[:, :1].astype(F32)
    target = jnp.where(
        slot_of < count, block[:, :1].astype(F32) * row_total + first + slot_of, -1.0
    )
    column = lax.broadcasted_iota(jnp.int32, (slots, blocks * row_total), 1).astype(F32)
    weight = None
    if weight_ref is not None:
        weight = jnp.sum(jnp.where(match, weight_ref[...], 0.0), axis=1, keepdims=True)
    return column == target, weight


def owner_of(step, owners):
    plane = plane_of(owners)
    me = lax.axis_index("expert")
    return (me // plane) * plane + ((me % plane) ^ step)


def select_kernel(owners, local_count, weighted, *refs):
    plane = plane_of(owners)
    blocks = owners // plane
    block_refs, aux_refs = refs[:blocks], refs[blocks : 2 * blocks]
    weight_ref = refs[2 * blocks] if weighted else None
    out_refs = refs[-plane:]
    row_total = block_refs[0].shape[0]
    for m in range(plane):
        chosen, weight = slot_map(
            aux_refs, weight_ref, owner_of(m, owners) * local_count, local_count, row_total
        )
        chosen = chosen.astype(F32).astype(BF)
        picked = None
        for b in range(blocks):
            part = jnp.dot(
                chosen[:, b * row_total : (b + 1) * row_total],
                block_refs[b][...],
                preferred_element_type=F32,
            )
            picked = part if picked is None else picked + part
        if weighted:
            picked = picked * weight
        out_refs[m][...] = picked.astype(BF)


def aux_spec(row_total, width):
    return pl.BlockSpec((AUX, width), lambda i: (row_total // AUX, 0))


def whole(shape):
    return pl.BlockSpec(shape, lambda i: (0,) * len(shape))


def select(blocks, aux_blocks, weights, owners, local_count, row_total):
    plane = plane_of(owners)
    width = blocks[0].shape[1]
    slots = local_count * len(blocks) * CAP
    args = list(blocks) + list(aux_blocks)
    specs = [whole((row_total, width))] * len(blocks) + [aux_spec(row_total, width)] * len(blocks)
    if weights is not None:
        args.append(weights)
        specs.append(whole(weights.shape))
    return pl.pallas_call(
        functools.partial(select_kernel, owners, local_count, weights is not None),
        grid=(1,),
        out_shape=[jax.ShapeDtypeStruct((slots, width), BF)] * plane,
        in_specs=specs,
        out_specs=[whole((slots, width))] * plane,
        compiler_params=params(),
        cost_estimate=cost(
            2 * plane * slots * len(blocks) * row_total * width,
            2 * width * (plane * slots + len(blocks) * row_total),
        ),
        name="select",
    )(*args)


def combine_kernel(owners, local_count, weighted, row_total, *refs):
    plane = plane_of(owners)
    blocks = owners // plane
    slot_refs, aux_refs = refs[:plane], refs[plane : plane + blocks]
    weight_ref = refs[plane + blocks] if weighted else None
    out_refs = refs[-blocks:]
    total = None
    contract = (((0,), (0,)), ((), ()))
    for m in range(plane):
        chosen, weight = slot_map(
            aux_refs, weight_ref, owner_of(m, owners) * local_count, local_count, row_total
        )
        values = slot_refs[m][...]
        if weighted:
            full = jnp.where(chosen, weight, 0.0)
            high = full.astype(BF)
            low = (full - high.astype(F32)).astype(BF)
            terms = (high, low)
        else:
            terms = (chosen.astype(F32).astype(BF),)
        for term in terms:
            part = lax.dot_general(term, values, contract, preferred_element_type=F32)
            total = part if total is None else total + part
    for b in range(blocks):
        out_refs[b][...] = total[b * row_total : (b + 1) * row_total].astype(out_refs[b].dtype)


def combine(slots_in, aux_blocks, weights, owners, local_count, row_total):
    plane = plane_of(owners)
    blocks = owners // plane
    slots, width = slots_in[0].shape
    args = list(slots_in) + list(aux_blocks)
    specs = [whole((slots, width))] * plane + [aux_spec(row_total, width)] * blocks
    if weights is not None:
        args.append(weights)
        specs.append(whole(weights.shape))
    return pl.pallas_call(
        functools.partial(combine_kernel, owners, local_count, weights is not None, row_total),
        grid=(1,),
        out_shape=[
            jax.ShapeDtypeStruct((row_total, width), F32 if b == 0 else BF) for b in range(blocks)
        ],
        in_specs=specs,
        out_specs=[whole((row_total, width))] * blocks,
        compiler_params=params(),
        cost_estimate=cost(
            4 * plane * slots * blocks * row_total * width,
            2 * width * (plane * slots + blocks * row_total),
        ),
        name="combine",
    )(*args)


def gathered(refs, local_count, out_ref):
    group = refs[0].shape[0] // local_count
    values = [r[...].astype(F32) for r in refs]
    for e in range(local_count):
        out_ref[e] = jnp.concatenate(
            [v[e * group : (e + 1) * group] for v in values], axis=0
        ).astype(BF)


def scattered(total_ref, local_count, out_refs):
    group = out_refs[0].shape[0] // local_count
    for m, out_ref in enumerate(out_refs):
        out_ref[...] = jnp.concatenate(
            [total_ref[e, m * group : (m + 1) * group, :] for e in range(local_count)], axis=0
        ).astype(BF)


def forward_kernel(plane, local_count, *refs):
    slot_refs, (up_ref, down_ref) = refs[:plane], refs[plane : plane + 2]
    out_refs = refs[plane + 2 : 2 * plane + 2]
    pre_ref, act_ref, in_ref, total_ref = refs[2 * plane + 2 :]
    e, f = pl.program_id(0), pl.program_id(1)

    @pl.when((e == 0) & (f == 0))
    def _():
        gathered(slot_refs, local_count, in_ref)

    pre = jnp.dot(in_ref[e], up_ref[...], preferred_element_type=F32)
    act = (pre * (1.0 / (1.0 + jnp.exp(-pre)))).astype(BF)
    pre_ref[0] = pre
    act_ref[0] = act
    part = jnp.dot(act, down_ref[...], preferred_element_type=F32)

    @pl.when(f == 0)
    def _():
        total_ref[e] = part

    @pl.when(f > 0)
    def _():
        total_ref[e] += part

    @pl.when((e == local_count - 1) & (f == pl.num_programs(1) - 1))
    def _():
        scattered(total_ref, local_count, out_refs)


TILE = 512


def forward(slots_in, up_proj, down_proj, local_count):
    plane = len(slots_in)
    slots, width = slots_in[0].shape
    rows = slots * plane // local_count
    units = up_proj.shape[1] // local_count
    tiles = units // TILE
    held = pl.BlockSpec((slots, width), lambda e, f: (0, 0))
    return pl.pallas_call(
        functools.partial(forward_kernel, plane, local_count),
        grid=(local_count, tiles),
        out_shape=[jax.ShapeDtypeStruct((slots, width), BF)] * plane
        + [
            jax.ShapeDtypeStruct((local_count, rows, units), F32),
            jax.ShapeDtypeStruct((local_count, rows, units), BF),
            jax.ShapeDtypeStruct((local_count, rows, width), BF),
        ],
        in_specs=[held] * plane
        + [
            pl.BlockSpec((width, TILE), lambda e, f: (0, e * tiles + f)),
            pl.BlockSpec((TILE, width), lambda e, f: (e * tiles + f, 0)),
        ],
        out_specs=[held] * plane
        + [
            pl.BlockSpec((1, rows, TILE), lambda e, f: (e, 0, f)),
            pl.BlockSpec((1, rows, TILE), lambda e, f: (e, 0, f)),
            pl.BlockSpec((local_count, rows, width), lambda e, f: (0, 0, 0)),
        ],
        scratch_shapes=[pltpu.VMEM((local_count, rows, width), F32)],
        compiler_params=params(),
        cost_estimate=cost(4 * local_count * rows * width * units, 4 * up_proj.size),
        name="forward",
    )(*slots_in, up_proj, down_proj)


def backward_kernel(plane, local_count, *refs):
    slot_refs, (up_ref, down_ref, pre_ref) = refs[:plane], refs[plane : plane + 3]
    out_refs = refs[plane + 3 : 2 * plane + 3]
    pg_ref, in_ref, total_ref = refs[2 * plane + 3 :]
    e, f = pl.program_id(0), pl.program_id(1)

    @pl.when((e == 0) & (f == 0))
    def _():
        gathered(slot_refs, local_count, in_ref)

    contract = (((1,), (1,)), ((), ()))
    act_grad = lax.dot_general(in_ref[e], down_ref[...], contract, preferred_element_type=F32)
    pre = pre_ref[0]
    sg = 1.0 / (1.0 + jnp.exp(-pre))
    pre_grad = (act_grad * sg * (1.0 + pre * (1.0 - sg))).astype(BF)
    pg_ref[0] = pre_grad
    part = lax.dot_general(pre_grad, up_ref[...], contract, preferred_element_type=F32)

    @pl.when(f == 0)
    def _():
        total_ref[e] = part

    @pl.when(f > 0)
    def _():
        total_ref[e] += part

    @pl.when((e == local_count - 1) & (f == pl.num_programs(1) - 1))
    def _():
        scattered(total_ref, local_count, out_refs)


def backward(slots_in, up_proj, down_proj, pre, local_count):
    plane = len(slots_in)
    slots, width = slots_in[0].shape
    rows = slots * plane // local_count
    units = up_proj.shape[1] // local_count
    tiles = units // TILE
    held = pl.BlockSpec((slots, width), lambda e, f: (0, 0))
    return pl.pallas_call(
        functools.partial(backward_kernel, plane, local_count),
        grid=(local_count, tiles),
        out_shape=[jax.ShapeDtypeStruct((slots, width), BF)] * plane
        + [
            jax.ShapeDtypeStruct((local_count, rows, units), BF),
            jax.ShapeDtypeStruct((local_count, rows, width), BF),
        ],
        in_specs=[held] * plane
        + [
            pl.BlockSpec((width, TILE), lambda e, f: (0, e * tiles + f)),
            pl.BlockSpec((TILE, width), lambda e, f: (e * tiles + f, 0)),
            pl.BlockSpec((1, rows, TILE), lambda e, f: (e, 0, f)),
        ],
        out_specs=[held] * plane
        + [
            pl.BlockSpec((1, rows, TILE), lambda e, f: (e, 0, f)),
            pl.BlockSpec((local_count, rows, width), lambda e, f: (0, 0, 0)),
        ],
        scratch_shapes=[pltpu.VMEM((local_count, rows, width), F32)],
        compiler_params=params(),
        cost_estimate=cost(4 * local_count * rows * width * units, 4 * up_proj.size),
        name="backward",
    )(*slots_in, up_proj, down_proj, pre)


def outer_kernel(a_ref, b_ref, out_ref):
    out_ref[...] = lax.dot_general(
        a_ref[0], b_ref[0], (((0,), (0,)), ((), ())), preferred_element_type=F32
    ).astype(BF)


def down_outer(act, scaled):
    local_count, rows, units = act.shape
    width = scaled.shape[2]
    tiles = units // TILE
    return pl.pallas_call(
        outer_kernel,
        grid=(local_count, tiles),
        out_shape=jax.ShapeDtypeStruct((local_count * units, width), BF),
        in_specs=[
            pl.BlockSpec((1, rows, TILE), lambda e, f: (e, 0, f)),
            pl.BlockSpec((1, rows, width), lambda e, f: (e, 0, 0)),
        ],
        out_specs=pl.BlockSpec((TILE, width), lambda e, f: (e * tiles + f, 0)),
        compiler_params=params(),
        cost_estimate=cost(2 * local_count * rows * width * units, 2 * local_count * units * width),
        name="down_outer",
    )(act, scaled)


def up_outer(inputs, pre_grad):
    local_count, rows, width = inputs.shape
    units = pre_grad.shape[2]
    tiles = units // TILE
    return pl.pallas_call(
        outer_kernel,
        grid=(local_count, tiles),
        out_shape=jax.ShapeDtypeStruct((width, local_count * units), BF),
        in_specs=[
            pl.BlockSpec((1, rows, width), lambda e, f: (e, 0, 0)),
            pl.BlockSpec((1, rows, TILE), lambda e, f: (e, 0, f)),
        ],
        out_specs=pl.BlockSpec((width, TILE), lambda e, f: (0, e * tiles + f)),
        compiler_params=params(),
        cost_estimate=cost(2 * local_count * rows * width * units, 2 * local_count * units * width),
        name="up_outer",
    )(inputs, pre_grad)


def spread(block, owners, plane):
    held = [block]
    mask = owners // 2
    received = {0: block}
    while mask >= plane:
        for k in list(received):
            received[k | mask] = hop(received[k], mask, owners)
        mask //= 2
    return [received[k * plane] for k in range(owners // plane)]


def gather_sum(parts, owners, plane):
    held = {k * plane: part for k, part in enumerate(parts)}
    mask = plane
    while mask < owners:
        for k in [k for k in held if k & mask]:
            got = hop(held.pop(k).astype(BF), mask, owners).astype(F32)
            base = k ^ mask
            held[base] = held[base].astype(F32) + got
        mask *= 2
    return held[0]


def in_plane(parts, owners):
    return [part if m == 0 else hop(part, m, owners) for m, part in enumerate(parts)]


def per_device_planes(rows, cotangent, up_proj, down_proj, mix_weight, task_counts, expert_order):
    owners = lax.axis_size("expert")
    plane = plane_of(owners)
    row_total, _ = rows.shape
    local_count = up_proj.shape[1] // FF
    weights = jnp.pad(mix_weight.reshape(1, -1), ((0, 0), (0, LANES - EXPERTS)))

    tagged = spread(prep(rows, task_counts, expert_order), owners, plane)
    grads = spread(cotangent, owners, plane)
    got_rows = in_plane(select(tagged, tagged, None, owners, local_count, row_total), owners)
    got_grads = in_plane(select(grads, tagged, weights, owners, local_count, row_total), owners)

    *outputs, pre, act, inputs = forward(got_rows, up_proj, down_proj, local_count)
    back_out = in_plane(outputs, owners)
    *input_grads, pre_grad, scaled = backward(got_grads, up_proj, down_proj, pre, local_count)
    back_grads = in_plane(input_grads, owners)
    down_grad = down_outer(act, scaled)
    up_grad = up_outer(inputs, pre_grad)

    mixed = gather_sum(
        combine(back_out, tagged, weights, owners, local_count, row_total), owners, plane
    ).astype(BF)
    row_gradient = gather_sum(
        combine(back_grads, tagged, None, owners, local_count, row_total), owners, plane
    ).astype(BF)
    return (mixed, row_gradient, up_grad, down_grad)


def block_route(counts, expert_list, mix_flat, row_total):
    firsts = jnp.cumsum(counts) - counts
    labels = jnp.arange(EXPERTS, dtype=jnp.int32)
    matches = expert_list[None, :] == labels[:, None]
    position = jnp.sum(jnp.where(matches, labels[None, :], 0), axis=1)
    task_of = position // K
    task_match = task_of[:, None] == jnp.arange(TASKS, dtype=jnp.int32)[None, :]
    count_of = jnp.sum(jnp.where(task_match, counts[None, :], 0), axis=1)
    first_of = jnp.sum(jnp.where(task_match, firsts[None, :], 0), axis=1)
    weight_of = jnp.sum(
        jnp.where(matches, mix_flat[None, :], jnp.zeros_like(mix_flat)[None, :]), axis=1
    )
    slot_index = jnp.arange(CAP, dtype=jnp.int32)
    filled = slot_index[None, :] < count_of[:, None]
    targets = first_of[:, None] + slot_index[None, :]
    row_index = jnp.arange(row_total, dtype=jnp.int32)
    selection_index = (targets[:, :, None] == row_index[None, None, :]) & filled[:, :, None]
    selection_index = selection_index.reshape(EXPERTS * CAP, row_total).astype(jnp.float32)
    slot_weight = jnp.where(filled, weight_of[:, None], jnp.zeros_like(weight_of)[:, None]).reshape(
        -1
    )
    return (selection_index, slot_weight)


def to_owners(values, copies, owners):
    if copies > 1:
        return jnp.repeat(values, copies, axis=0)
    return values.reshape((owners, -1) + values.shape[2:])


def from_owners(values, copies, hidden_width):
    if copies > 1:
        return jnp.sum(values.reshape(EXPERTS, copies, CAP, hidden_width), axis=1)
    return values.reshape(EXPERTS, CAP, hidden_width)


def forward_part(got_rows, up_local, down_local, owners, local_count, slot_count):
    hidden_width = got_rows.shape[-1]
    inputs = got_rows.reshape(owners, local_count, slot_count, hidden_width)
    pre = jnp.einsum("nlcd,dlf->nlcf", inputs, up_local, preferred_element_type=jnp.float32)
    act = jax.nn.silu(pre).astype(jnp.bfloat16)
    outputs = jnp.einsum("nlcf,lfd->nlcd", act, down_local, preferred_element_type=jnp.float32)
    return (inputs, pre, act, outputs.reshape(owners, local_count * slot_count, hidden_width))


def backward_part(
    inputs, got_grads, pre, act, up_local, down_local, owners, local_count, slot_count
):
    hidden_width = inputs.shape[-1]
    scaled = got_grads.reshape(owners, local_count, slot_count, hidden_width)
    act_grad = jnp.einsum("nlcd,lfd->nlcf", scaled, down_local, preferred_element_type=jnp.float32)
    sigmoid = jax.nn.sigmoid(pre)
    pre_grad = (act_grad * sigmoid * (1.0 + pre * (1.0 - sigmoid))).astype(jnp.bfloat16)
    down_grad = jnp.einsum("nlcf,nlcd->lfd", act, scaled, preferred_element_type=jnp.float32)
    up_grad = jnp.einsum("nlcd,nlcf->dlf", inputs, pre_grad, preferred_element_type=jnp.float32)
    partial_grads = jnp.einsum(
        "nlcf,dlf->nlcd", pre_grad, up_local, preferred_element_type=jnp.float32
    )
    units = up_local.shape[1] * up_local.shape[2]
    return (
        up_grad.reshape(hidden_width, units),
        down_grad.reshape(units, hidden_width),
        partial_grads.reshape(owners, local_count * slot_count, hidden_width),
    )


def per_device_direct(rows, cotangent, up_proj, down_proj, mix_weight, task_counts, expert_order):
    owners = lax.axis_size("expert")
    row_total = rows.shape[0]
    hidden_width = rows.shape[1]
    units = up_proj.shape[1]
    local_units = min(units, FF)
    local_count = max(units // FF, 1)
    copies = max(FF // units, 1)
    selection_index, slot_weight = block_route(
        task_counts[0], expert_order[0], mix_weight.reshape(-1), row_total
    )
    select_half = selection_index.astype(jnp.bfloat16)
    slot_row_values = jnp.dot(select_half, rows, preferred_element_type=jnp.float32).astype(
        jnp.bfloat16
    )
    slot_gradient_rows = jnp.dot(select_half, cotangent, preferred_element_type=jnp.float32)
    scaled = (slot_weight[:, None] * slot_gradient_rows).astype(jnp.bfloat16)
    upper_bound = lax.Precision.HIGHEST
    sent_rows = to_owners(slot_row_values.reshape(EXPERTS, CAP, hidden_width), copies, owners)
    sent_grads = to_owners(scaled.reshape(EXPERTS, CAP, hidden_width), copies, owners)
    up_local = up_proj.reshape(hidden_width, local_count, local_units)
    down_local = down_proj.reshape(local_count, local_units, hidden_width)
    got_rows = lax.all_to_all(sent_rows, "expert", split_axis=0, concat_axis=0, tiled=True)
    inputs, pre, act, outputs = forward_part(
        got_rows, up_local, down_local, owners, local_count, CAP
    )
    back_out = lax.all_to_all(outputs, "expert", split_axis=0, concat_axis=0, tiled=True)
    got_grads = lax.all_to_all(sent_grads, "expert", split_axis=0, concat_axis=0, tiled=True)
    up_full, down_full, partial_grads = backward_part(
        inputs, got_grads, pre, act, up_local, down_local, owners, local_count, CAP
    )
    back_grads = lax.all_to_all(partial_grads, "expert", split_axis=0, concat_axis=0, tiled=True)
    up_grad = up_full.astype(jnp.bfloat16)
    down_grad = down_full.astype(jnp.bfloat16)
    returned = from_owners(back_out, copies, hidden_width).reshape(EXPERTS * CAP, hidden_width)
    summed_grads = from_owners(back_grads, copies, hidden_width).reshape(
        EXPERTS * CAP, hidden_width
    )
    weighted_rows = returned * slot_weight[:, None]
    mixed = jnp.dot(selection_index.T, weighted_rows, precision=upper_bound).astype(jnp.bfloat16)
    row_gradient = jnp.dot(selection_index.T, summed_grads, precision=upper_bound).astype(
        jnp.bfloat16
    )
    return (mixed, row_gradient, up_grad, down_grad)


def per_device(rows, cotangent, up_proj, *rest):
    owners = lax.axis_size("expert")
    planes = up_proj.shape[1] % FF == 0 and owners & (owners - 1) == 0 and owners > 1
    return (per_device_planes if planes else per_device_direct)(rows, cotangent, up_proj, *rest)


def solution(mesh):
    return jax.shard_map(
        per_device,
        mesh=mesh,
        in_specs=(
            P(("group", "expert"), None),
            P(("group", "expert"), None),
            P(None, "expert"),
            P("expert", None),
            P(),
            P(("group", "expert"), None),
            P(("group", "expert"), None),
        ),
        out_specs=(
            P(("group", "expert"), None),
            P(("group", "expert"), None),
            P("group", "expert"),
            P("expert", "group"),
        ),
        check_vma=False,
    )
```

```python
import functools

import jax
import jax.numpy as jnp
from jax import lax
from jax.experimental import pallas as pl
from jax.experimental.pallas import tpu as pltpu
from jax.sharding import PartitionSpec as P


FF = 2048
EXPERTS = 32
TASKS = 8
K = 4
CAP = 18
AUX = 8
LANES = 128
TILE = 1024
HALVES = 2
TOUCHES = 3
BF = jnp.bfloat16
F32 = jnp.float32


def plane_of(owners):
    return 1 << ((owners.bit_length() - 1) // 2)


def parts_of(blocks):
    count = min(HALVES, blocks)
    step = blocks // count
    return [tuple(range(i * step, (i + 1) * step)) for i in range(count)]


def hop(value, mask, owners):
    return lax.ppermute(value, "expert", [(i, i ^ mask) for i in range(owners)])


def params(limit_mib=16):
    return pltpu.CompilerParams(vmem_limit_bytes=limit_mib << 20)


def cost(flops, moved):
    return pl.CostEstimate(flops=int(flops), bytes_accessed=int(moved), transcendentals=0)


def in_vmem():
    return pl.BlockSpec(memory_space=pltpu.VMEM)


def whole(shape):
    return pl.BlockSpec(shape, lambda i: (0,) * len(shape))


def prep_kernel(counts_ref, order_ref, out_ref):
    lane = lax.broadcasted_iota(jnp.int32, (1, LANES), 1)
    first_of = jnp.zeros((1, LANES), jnp.int32)
    count_of = jnp.zeros((1, LANES), jnp.int32)
    total = jnp.int32(0)
    for t in range(TASKS):
        here = (lane >= t * K) & (lane < (t + 1) * K)
        count = counts_ref[0, t]
        first_of = jnp.where(here, total, first_of)
        count_of = jnp.where(here, count, count_of)
        total = total + count
    order = jnp.concatenate(
        [order_ref[...], jnp.full((1, LANES - EXPERTS), -1, jnp.int32)], axis=1
    )
    sub = lax.broadcasted_iota(jnp.int32, (AUX, LANES), 0)
    aux = jnp.where(
        sub == 0, order, jnp.where(sub == 1, first_of, jnp.where(sub == 2, count_of, 0))
    )
    out_ref[...] = aux.astype(F32).astype(BF)


def prep(counts, order):
    return pl.pallas_call(
        prep_kernel,
        grid=(1,),
        out_shape=jax.ShapeDtypeStruct((AUX, LANES), BF),
        in_specs=[
            pl.BlockSpec(counts.shape, lambda i: (0, 0), memory_space=pltpu.SMEM),
            whole(order.shape),
        ],
        out_specs=whole((AUX, LANES)),
        compiler_params=params(),
        cost_estimate=cost(1e6, 4096),
    )(counts, order)


def touch_kernel(up_ref, down_ref, out_ref):
    out_ref[...] = up_ref[:8, :LANES] + down_ref[:8, :LANES]


def touch(up_proj, down_proj):
    return pl.pallas_call(
        touch_kernel,
        out_shape=jax.ShapeDtypeStruct((8, LANES), BF),
        in_specs=[in_vmem()] * 2,
        out_specs=in_vmem(),
        compiler_params=pltpu.CompilerParams(
            vmem_limit_bytes=16 << 20, has_side_effects=True
        ),
        cost_estimate=cost(1e9, 4 * up_proj.size),
    )(up_proj, down_proj)


def slot_map(aux_refs, weight_ref, first_expert, local_count, row_total):
    blocks = len(aux_refs)
    group = blocks * CAP
    slots = local_count * group
    q = lax.broadcasted_iota(jnp.int32, (slots, LANES), 0)
    expert = block = jnp.zeros_like(q)
    for e in range(1, local_count):
        expert = expert + (q >= e * group).astype(jnp.int32)
    rest = q - expert * group
    for b in range(1, blocks):
        block = block + (rest >= b * CAP).astype(jnp.int32)
    slot = rest - block * CAP
    order = first = count = jnp.zeros((slots, LANES), F32)
    for b in range(blocks):
        aux = aux_refs[b][...].astype(F32)
        order = jnp.where(block == b, aux[0:1, :LANES], order)
        first = jnp.where(block == b, aux[1:2, :LANES], first)
        count = jnp.where(block == b, aux[2:3, :LANES], count)
    match = order == (expert + first_expert).astype(F32)
    first = jnp.sum(jnp.where(match, first, 0.0), axis=1, keepdims=True)
    count = jnp.sum(jnp.where(match, count, 0.0), axis=1, keepdims=True)
    slot_of = slot[:, :1].astype(F32)
    target = jnp.where(
        slot_of < count, block[:, :1].astype(F32) * row_total + first + slot_of, -1.0
    )
    column = lax.broadcasted_iota(jnp.int32, (slots, blocks * row_total), 1).astype(F32)
    weight = None
    if weight_ref is not None:
        weight = jnp.sum(jnp.where(match, weight_ref[...], 0.0), axis=1, keepdims=True)
    return column == target, weight


def owner_of(step, owners):
    plane = plane_of(owners)
    me = lax.axis_index("expert")
    return (me // plane) * plane + ((me % plane) ^ step)


def select_kernel(owners, local_count, weighted, blocks, *refs):
    plane = plane_of(owners)
    block_refs, aux_refs = refs[:blocks], refs[blocks : 2 * blocks]
    weight_ref = refs[2 * blocks] if weighted else None
    out_refs = refs[-plane:]
    row_total = block_refs[0].shape[0]
    for m in range(plane):
        chosen, weight = slot_map(
            aux_refs, weight_ref, owner_of(m, owners) * local_count, local_count, row_total
        )
        chosen = chosen.astype(F32).astype(BF)
        picked = None
        for b in range(blocks):
            part = jnp.dot(
                chosen[:, b * row_total : (b + 1) * row_total],
                block_refs[b][...],
                preferred_element_type=F32,
            )
            picked = part if picked is None else picked + part
        if weighted:
            picked = picked * weight
        out_refs[m][...] = picked.astype(BF)


def select(blocks, aux_blocks, weights, owners, local_count, row_total):
    plane = plane_of(owners)
    width = blocks[0].shape[1]
    slots = local_count * len(blocks) * CAP
    args = list(blocks) + list(aux_blocks)
    specs = [whole((row_total, width))] * len(blocks) + [whole((AUX, LANES))] * len(blocks)
    if weights is not None:
        args.append(weights)
        specs.append(whole(weights.shape))
    return pl.pallas_call(
        functools.partial(
            select_kernel, owners, local_count, weights is not None, len(blocks)
        ),
        grid=(1,),
        out_shape=[jax.ShapeDtypeStruct((slots, width), BF)] * plane,
        in_specs=specs,
        out_specs=[whole((slots, width))] * plane,
        compiler_params=params(),
        cost_estimate=cost(
            2 * plane * slots * len(blocks) * row_total * width,
            2 * width * (plane * slots + len(blocks) * row_total),
        ),
    )(*args)


def combine_kernel(owners, local_count, weighted, row_total, blocks, *refs):
    plane = plane_of(owners)
    slot_refs, aux_refs = refs[:plane], refs[plane : plane + blocks]
    weight_ref = refs[plane + blocks] if weighted else None
    out_refs = refs[-blocks:]
    chosen_all, values_all = [], []
    for m in range(plane):
        chosen, weight = slot_map(
            aux_refs, weight_ref, owner_of(m, owners) * local_count, local_count, row_total
        )
        values = slot_refs[m][...].astype(F32)
        if weighted:
            values = values * weight
        chosen_all.append(chosen.astype(F32))
        values_all.append(values)
    total = lax.dot_general(
        jnp.concatenate(chosen_all, axis=0).astype(BF),
        jnp.concatenate(values_all, axis=0).astype(BF),
        (((0,), (0,)), ((), ())),
        preferred_element_type=F32,
    )
    for b in range(blocks):
        out_refs[b][...] = total[b * row_total : (b + 1) * row_total].astype(out_refs[b].dtype)


def combine(slots_in, aux_blocks, weights, owners, local_count, row_total, own):
    plane = plane_of(owners)
    blocks = len(aux_blocks)
    slots, width = slots_in[0].shape
    args = list(slots_in) + list(aux_blocks)
    specs = [whole((slots, width))] * plane + [whole((AUX, LANES))] * blocks
    if weights is not None:
        args.append(weights)
        specs.append(whole(weights.shape))
    return pl.pallas_call(
        functools.partial(
            combine_kernel, owners, local_count, weights is not None, row_total, blocks
        ),
        grid=(1,),
        out_shape=[
            jax.ShapeDtypeStruct((row_total, width), F32 if own and b == 0 else BF)
            for b in range(blocks)
        ],
        in_specs=specs,
        out_specs=[whole((row_total, width))] * blocks,
        compiler_params=params(),
        cost_estimate=cost(
            2 * plane * slots * blocks * row_total * width,
            2 * width * (plane * slots + blocks * row_total),
        ),
    )(*args)


def gathered(slot_refs, e, local_count, wide_ref, out_ref):
    at = 0
    for ref in slot_refs:
        group = ref.shape[0] // local_count
        value = ref[...].astype(F32)
        wide_ref[at : at + group, :] = value[e * group : (e + 1) * group]
        at += group
    out_ref[...] = wide_ref[...].astype(BF)


def scattered(total_refs, out_refs, place_ref):
    local_count = len(total_refs)
    at = 0
    for out_ref in out_refs:
        group = out_ref.shape[0] // local_count
        for e, total_ref in enumerate(total_refs):
            place_ref[e * group : (e + 1) * group, :] = total_ref[at : at + group, :]
        out_ref[...] = place_ref[...].astype(BF)
        at += group


def shapes_of(slots_in, local_count, e):
    rows = sum(value.shape[0] for value in slots_in) // local_count
    width = slots_in[0].shape[1]
    if e < local_count - 1:
        return [jax.ShapeDtypeStruct((rows, width), F32)]
    return [jax.ShapeDtypeStruct(value.shape, BF) for value in slots_in]


def scratch_of(slots_in, local_count):
    rows = sum(value.shape[0] for value in slots_in) // local_count
    width = slots_in[0].shape[1]
    return [
        pltpu.VMEM((rows, width), F32),
        pltpu.VMEM((rows, width), F32),
        pltpu.VMEM((max(value.shape[0] for value in slots_in), width), F32),
    ]


def finish(total_ref, before_refs, result_refs, place_ref, local_count):
    if len(before_refs) < local_count - 1:
        result_refs[0][...] = total_ref[...]
    else:
        scattered([*before_refs, total_ref], result_refs, place_ref)


def forward_kernel(slot_count, local_count, e, *refs):
    slot_refs, (up_ref, down_ref) = refs[:slot_count], refs[slot_count : slot_count + 2]
    before_refs, rest = refs[slot_count + 2 : slot_count + 2 + e], refs[slot_count + 2 + e :]
    *result_refs, pre_ref, act_ref, in_ref, wide_ref, total_ref, place_ref = rest
    units = up_ref.shape[1] // local_count
    gathered(slot_refs, e, local_count, wide_ref, in_ref)

    def step(f):
        inner = pl.ds(f * TILE, TILE)
        outer = pl.ds(e * units + f * TILE, TILE)
        pre = jnp.dot(in_ref[...], up_ref[:, outer], preferred_element_type=F32)
        act = (pre * (1.0 / (1.0 + jnp.exp(-pre)))).astype(BF)
        pre_ref[:, inner] = pre
        act_ref[:, inner] = act
        part = jnp.dot(act, down_ref[outer, :], preferred_element_type=F32)
        total_ref[...] = part if f == 0 else total_ref[...] + part

    for f in range(units // TILE):
        step(f)
    finish(total_ref, before_refs, result_refs, place_ref, local_count)


def forward(slots_in, up_proj, down_proj, before, local_count, e):
    width = slots_in[0].shape[1]
    rows = sum(value.shape[0] for value in slots_in) // local_count
    units = up_proj.shape[1] // local_count
    args = [*slots_in, up_proj, down_proj, *before]
    out_shape = shapes_of(slots_in, local_count, e) + [
        jax.ShapeDtypeStruct((rows, units), F32),
        jax.ShapeDtypeStruct((rows, units), BF),
        jax.ShapeDtypeStruct((rows, width), BF),
    ]
    return pl.pallas_call(
        functools.partial(forward_kernel, len(slots_in), local_count, e),
        out_shape=out_shape,
        in_specs=[in_vmem()] * len(args),
        out_specs=[in_vmem()] * len(out_shape),
        scratch_shapes=scratch_of(slots_in, local_count),
        compiler_params=params(),
        cost_estimate=cost(4 * rows * width * units, 4 * up_proj.size // local_count),
    )(*args)


def backward_kernel(slot_count, local_count, e, *refs):
    slot_refs, (up_ref, down_ref, pre_ref) = refs[:slot_count], refs[slot_count : slot_count + 3]
    before_refs, rest = refs[slot_count + 3 : slot_count + 3 + e], refs[slot_count + 3 + e :]
    *result_refs, pg_ref, in_ref, wide_ref, total_ref, place_ref = rest
    units = up_ref.shape[1] // local_count
    gathered(slot_refs, e, local_count, wide_ref, in_ref)
    contract = (((1,), (1,)), ((), ()))

    def step(f):
        inner = pl.ds(f * TILE, TILE)
        outer = pl.ds(e * units + f * TILE, TILE)
        act_grad = lax.dot_general(
            in_ref[...], down_ref[outer, :], contract, preferred_element_type=F32
        )
        pre = pre_ref[:, inner]
        sg = 1.0 / (1.0 + jnp.exp(-pre))
        pre_grad = (act_grad * sg * (1.0 + pre * (1.0 - sg))).astype(BF)
        pg_ref[:, inner] = pre_grad
        part = lax.dot_general(pre_grad, up_ref[:, outer], contract, preferred_element_type=F32)
        total_ref[...] = part if f == 0 else total_ref[...] + part

    for f in range(units // TILE):
        step(f)
    finish(total_ref, before_refs, result_refs, place_ref, local_count)


def backward(slots_in, up_proj, down_proj, pre, before, local_count, e):
    width = slots_in[0].shape[1]
    rows = sum(value.shape[0] for value in slots_in) // local_count
    units = up_proj.shape[1] // local_count
    args = [*slots_in, up_proj, down_proj, pre, *before]
    out_shape = shapes_of(slots_in, local_count, e) + [
        jax.ShapeDtypeStruct((rows, units), BF),
        jax.ShapeDtypeStruct((rows, width), BF),
    ]
    return pl.pallas_call(
        functools.partial(backward_kernel, len(slots_in), local_count, e),
        out_shape=out_shape,
        in_specs=[in_vmem()] * len(args),
        out_specs=[in_vmem()] * len(out_shape),
        scratch_shapes=scratch_of(slots_in, local_count),
        compiler_params=params(),
        cost_estimate=cost(4 * rows * width * units, 4 * up_proj.size // local_count),
    )(*args)


def down_outer_kernel(act_ref, scaled_ref, *refs):
    refs[-1][...] = lax.dot_general(
        act_ref[...], scaled_ref[...], (((0,), (0,)), ((), ())), preferred_element_type=F32
    ).astype(BF)


def down_outer(act, scaled, before, e, local_count):
    rows, units = act.shape
    width = scaled.shape[1]
    tiles = units // TILE
    extra = [] if before is None else [before]
    return pl.pallas_call(
        down_outer_kernel,
        grid=(tiles,),
        out_shape=jax.ShapeDtypeStruct((local_count * units, width), BF),
        in_specs=[
            pl.BlockSpec((rows, TILE), lambda f: (0, f)),
            pl.BlockSpec((rows, width), lambda f: (0, 0)),
        ]
        + [pl.BlockSpec(memory_space=pl.ANY)] * len(extra),
        out_specs=pl.BlockSpec((TILE, width), lambda f: (e * tiles + f, 0)),
        input_output_aliases={2: 0} if extra else {},
        compiler_params=params(),
        cost_estimate=cost(2 * rows * width * units, 2 * units * width),
    )(act, scaled, *extra)


def up_outer_kernel(inputs_ref, pg_ref, *refs):
    out_ref, turned_ref = refs[-2:]

    @pl.when(pl.program_id(0) == 0)
    def _():
        turned_ref[...] = inputs_ref[...].T

    out_ref[...] = jnp.dot(turned_ref[...], pg_ref[...], preferred_element_type=F32).astype(BF)


def up_outer(inputs, pre_grad, before, e, local_count):
    rows, width = inputs.shape
    units = pre_grad.shape[1]
    tiles = units // TILE
    extra = [] if before is None else [before]
    return pl.pallas_call(
        up_outer_kernel,
        grid=(tiles,),
        out_shape=jax.ShapeDtypeStruct((width, local_count * units), BF),
        in_specs=[
            pl.BlockSpec((rows, width), lambda f: (0, 0)),
            pl.BlockSpec((rows, TILE), lambda f: (0, f)),
        ]
        + [pl.BlockSpec(memory_space=pl.ANY)] * len(extra),
        out_specs=pl.BlockSpec((width, TILE), lambda f: (0, e * tiles + f)),
        input_output_aliases={2: 0} if extra else {},
        scratch_shapes=[pltpu.VMEM((width, rows), BF)],
        compiler_params=params(),
        cost_estimate=cost(2 * rows * width * units, 2 * units * width),
    )(inputs, pre_grad, *extra)


def spread(block, owners, plane):
    mask = owners // 2
    received = {0: block}
    while mask >= plane:
        for k in list(received):
            received[k | mask] = hop(received[k], mask, owners)
        mask //= 2
    return [received[k * plane] for k in range(owners // plane)]


def gather_sum(parts, owners, plane):
    held = {k * plane: part for k, part in enumerate(parts)}
    mask = plane
    while mask < owners:
        for k in sorted((k for k in held if k & mask), reverse=True):
            got = hop(held.pop(k).astype(BF), mask, owners).astype(F32)
            held[k ^ mask] = held[k ^ mask].astype(F32) + got
        mask *= 2
    return held[0]


def in_plane(parts, owners):
    return [part if m == 0 else hop(part, m, owners) for m, part in enumerate(parts)]


def per_device_planes(rows, cotangent, up_proj, down_proj, mix_weight, task_counts, expert_order):
    owners = lax.axis_size("expert")
    plane = plane_of(owners)
    row_total, _ = rows.shape
    local_count = up_proj.shape[1] // FF
    weights = jnp.pad(mix_weight.reshape(1, -1), ((0, 0), (0, LANES - EXPERTS)))
    groups = parts_of(owners // plane)

    tags = spread(prep(task_counts, expert_order), owners, plane)
    blocks = spread(rows, owners, plane)
    grads = spread(cotangent, owners, plane)
    for _ in range(TOUCHES):
        touch(up_proj, down_proj)

    def exchanged(whole_blocks, factors):
        slots = []
        for group in groups:
            chosen = select(
                [whole_blocks[b] for b in group],
                [tags[b] for b in group],
                factors,
                owners,
                local_count,
                row_total,
            )
            slots += in_plane(chosen, owners)
        return slots

    def returned(slots, factors):
        parts = []
        for h, group in enumerate(groups):
            parts += combine(
                in_plane(slots[h * plane : (h + 1) * plane], owners),
                [tags[b] for b in group],
                factors,
                owners,
                local_count,
                row_total,
                h == 0,
            )
        return gather_sum(parts, owners, plane).astype(BF)

    got_rows = exchanged(blocks, None)
    got_grads = exchanged(grads, weights)
    results, before, kept = [], [], []
    for e in range(local_count):
        *results, pre, act, inputs = forward(got_rows, up_proj, down_proj, before, local_count, e)
        before = before + results
        kept.append((pre, act, inputs))
    mixed = returned(results, weights)
    before, down_grad, up_grad = [], None, None
    for e, (pre, act, inputs) in enumerate(kept):
        *results, pre_grad, scaled = backward(
            got_grads, up_proj, down_proj, pre, before, local_count, e
        )
        before = before + results
        down_grad = down_outer(act, scaled, down_grad, e, local_count)
        up_grad = up_outer(inputs, pre_grad, up_grad, e, local_count)
    row_gradient = returned(results, None)
    return (mixed, row_gradient, up_grad, down_grad)


def block_route(counts, expert_list, mix_flat, row_total):
    firsts = jnp.cumsum(counts) - counts
    labels = jnp.arange(EXPERTS, dtype=jnp.int32)
    matches = expert_list[None, :] == labels[:, None]
    position = jnp.sum(jnp.where(matches, labels[None, :], 0), axis=1)
    task_of = position // K
    task_match = task_of[:, None] == jnp.arange(TASKS, dtype=jnp.int32)[None, :]
    count_of = jnp.sum(jnp.where(task_match, counts[None, :], 0), axis=1)
    first_of = jnp.sum(jnp.where(task_match, firsts[None, :], 0), axis=1)
    weight_of = jnp.sum(
        jnp.where(matches, mix_flat[None, :], jnp.zeros_like(mix_flat)[None, :]), axis=1
    )
    slot_index = jnp.arange(CAP, dtype=jnp.int32)
    filled = slot_index[None, :] < count_of[:, None]
    targets = first_of[:, None] + slot_index[None, :]
    row_index = jnp.arange(row_total, dtype=jnp.int32)
    selection_index = (targets[:, :, None] == row_index[None, None, :]) & filled[:, :, None]
    selection_index = selection_index.reshape(EXPERTS * CAP, row_total).astype(jnp.float32)
    slot_weight = jnp.where(filled, weight_of[:, None], jnp.zeros_like(weight_of)[:, None]).reshape(
        -1
    )
    return (selection_index, slot_weight)


def to_owners(values, copies, owners):
    if copies > 1:
        return jnp.repeat(values, copies, axis=0)
    return values.reshape((owners, -1) + values.shape[2:])


def from_owners(values, copies, hidden_width):
    if copies > 1:
        return jnp.sum(values.reshape(EXPERTS, copies, CAP, hidden_width), axis=1)
    return values.reshape(EXPERTS, CAP, hidden_width)


def forward_part(got_rows, up_local, down_local, owners, local_count, slot_count):
    hidden_width = got_rows.shape[-1]
    inputs = got_rows.reshape(owners, local_count, slot_count, hidden_width)
    pre = jnp.einsum("nlcd,dlf->nlcf", inputs, up_local, preferred_element_type=jnp.float32)
    act = jax.nn.silu(pre).astype(jnp.bfloat16)
    outputs = jnp.einsum("nlcf,lfd->nlcd", act, down_local, preferred_element_type=jnp.float32)
    return (inputs, pre, act, outputs.reshape(owners, local_count * slot_count, hidden_width))


def backward_part(
    inputs, got_grads, pre, act, up_local, down_local, owners, local_count, slot_count
):
    hidden_width = inputs.shape[-1]
    scaled = got_grads.reshape(owners, local_count, slot_count, hidden_width)
    act_grad = jnp.einsum("nlcd,lfd->nlcf", scaled, down_local, preferred_element_type=jnp.float32)
    sigmoid = jax.nn.sigmoid(pre)
    pre_grad = (act_grad * sigmoid * (1.0 + pre * (1.0 - sigmoid))).astype(jnp.bfloat16)
    down_grad = jnp.einsum("nlcf,nlcd->lfd", act, scaled, preferred_element_type=jnp.float32)
    up_grad = jnp.einsum("nlcd,nlcf->dlf", inputs, pre_grad, preferred_element_type=jnp.float32)
    partial_grads = jnp.einsum(
        "nlcf,dlf->nlcd", pre_grad, up_local, preferred_element_type=jnp.float32
    )
    units = up_local.shape[1] * up_local.shape[2]
    return (
        up_grad.reshape(hidden_width, units),
        down_grad.reshape(units, hidden_width),
        partial_grads.reshape(owners, local_count * slot_count, hidden_width),
    )


def per_device_direct(rows, cotangent, up_proj, down_proj, mix_weight, task_counts, expert_order):
    owners = lax.axis_size("expert")
    row_total = rows.shape[0]
    hidden_width = rows.shape[1]
    units = up_proj.shape[1]
    local_units = min(units, FF)
    local_count = max(units // FF, 1)
    copies = max(FF // units, 1)
    selection_index, slot_weight = block_route(
        task_counts[0], expert_order[0], mix_weight.reshape(-1), row_total
    )
    select_half = selection_index.astype(jnp.bfloat16)
    slot_row_values = jnp.dot(select_half, rows, preferred_element_type=jnp.float32).astype(
        jnp.bfloat16
    )
    slot_gradient_rows = jnp.dot(select_half, cotangent, preferred_element_type=jnp.float32)
    scaled = (slot_weight[:, None] * slot_gradient_rows).astype(jnp.bfloat16)
    upper_bound = lax.Precision.HIGHEST
    sent_rows = to_owners(slot_row_values.reshape(EXPERTS, CAP, hidden_width), copies, owners)
    sent_grads = to_owners(scaled.reshape(EXPERTS, CAP, hidden_width), copies, owners)
    up_local = up_proj.reshape(hidden_width, local_count, local_units)
    down_local = down_proj.reshape(local_count, local_units, hidden_width)
    got_rows = lax.all_to_all(sent_rows, "expert", split_axis=0, concat_axis=0, tiled=True)
    inputs, pre, act, outputs = forward_part(
        got_rows, up_local, down_local, owners, local_count, CAP
    )
    back_out = lax.all_to_all(outputs, "expert", split_axis=0, concat_axis=0, tiled=True)
    got_grads = lax.all_to_all(sent_grads, "expert", split_axis=0, concat_axis=0, tiled=True)
    up_full, down_full, partial_grads = backward_part(
        inputs, got_grads, pre, act, up_local, down_local, owners, local_count, CAP
    )
    back_grads = lax.all_to_all(partial_grads, "expert", split_axis=0, concat_axis=0, tiled=True)
    up_grad = up_full.astype(jnp.bfloat16)
    down_grad = down_full.astype(jnp.bfloat16)
    returned = from_owners(back_out, copies, hidden_width).reshape(EXPERTS * CAP, hidden_width)
    summed_grads = from_owners(back_grads, copies, hidden_width).reshape(
        EXPERTS * CAP, hidden_width
    )
    weighted_rows = returned * slot_weight[:, None]
    mixed = jnp.dot(selection_index.T, weighted_rows, precision=upper_bound).astype(jnp.bfloat16)
    row_gradient = jnp.dot(selection_index.T, summed_grads, precision=upper_bound).astype(
        jnp.bfloat16
    )
    return (mixed, row_gradient, up_grad, down_grad)


def takes_planes(owners, units):
    return units % FF == 0 and owners & (owners - 1) == 0 and owners > 1


def per_device(rows, cotangent, up_proj, *rest):
    if takes_planes(lax.axis_size("expert"), up_proj.shape[1]):
        return per_device_planes(rows, cotangent, up_proj, *rest)
    return per_device_direct(rows, cotangent, up_proj, *rest)


def solution(mesh):
    return jax.shard_map(
        per_device,
        mesh=mesh,
        in_specs=(
            P(("group", "expert"), None),
            P(("group", "expert"), None),
            P(None, "expert"),
            P("expert", None),
            P(),
            P(("group", "expert"), None),
            P(("group", "expert"), None),
        ),
        out_specs=(
            P(("group", "expert"), None),
            P(("group", "expert"), None),
            P("group", "expert"),
            P("expert", "group"),
        ),
        check_vma=False,
    )
```
